32 devices in a mesh: dom: 8 (over z, y), ray: 4 (over x, core).
Axes of the slice: x: 2, y: 2, z: 4, core: 2. Of those that a mesh axis runs over, the one named last changes fastest.
Arguments:
- projections: bfloat16 [8, 64, 8192], P('dom', None, 'ray'), may hold values from -6 to 6
- phase_kernel: bfloat16 [129], replicated, may hold values from -0.5 to 0.5
- image: bfloat16 [16384, 64], P('dom'), may hold values from -6 to 6
- tile_library: bfloat16 [8, 4, 16, 128, 128], P('dom', 'ray'), may hold values from -0.09375 to 0.09375
- tile_entry: int32 [8, 4, 256], P('dom', 'ray'), may hold values from 0 to 15
- tile_image: int32 [8, 4, 256], P('dom', 'ray'), may hold values from 0 to 15
- tile_slot: int32 [8, 4, 256], P('dom', 'ray'), may hold values from 0 to 7
- tile_count: int32 [8, 4], P('dom', 'ray'), may hold values from 64 to 256, as said below
- slot_block: int32 [8, 4, 8], P('dom', 'ray'), may hold values from 0 to 15
Outputs:
- residual: bfloat16 [8, 64, 8192], P('dom', None, 'ray')
- image_next: float32 [16384, 64], P(('dom', 'ray'))
The draws below stay inside these ranges and needn't reach their ends.
Inputs may be any that keep to these rules, and one draw needn't show every extreme that they name: `tile_count`: each device has at most 256 live tiles; some device holds exactly 256. Entries beyond a device's count are not used.
All inputs are finite; a program needn't handle non-finite values.
Results may differ from the reference program's by a relative error of at most 0.0075.
Values may be sent and summed in bfloat16 or wider, within the bound.
A program may use at most 64 MiB of HBM per device.

```python
import jax
import jax.numpy as jnp
from jax import lax

DET = 8192
TILE = 128
HALF = 64
SMOOTH = 8
ANG_DEV = 1
SLICES = 64
IB_DEV = 16
TILE_CAP = 256
LIB = 16
NA = 8
RAY_BLOCKS = 16
PIX = 16384
N_DOM = 8
N_RAY = 4


def draw_projections(key, part):
    background_key, stripe_key = jax.random.split(jax.random.fold_in(key, 11), 2)
    background = jnp.clip(jax.random.normal(background_key, (NA, SLICES, DET), jnp.float32), -4.0, 4.0)
    stripes = jnp.clip(jax.random.normal(stripe_key, (1, SLICES, DET), jnp.float32), -2.0, 2.0)
    return (background + stripes).astype(jnp.bfloat16)


def draw_tile_count(key, part):
    divisor_key, busiest_key = jax.random.split(jax.random.fold_in(key, 7))
    divisor = jax.random.randint(divisor_key, (N_DOM * N_RAY,), 1, 5)
    counts = TILE_CAP // divisor
    busiest = jax.random.randint(busiest_key, (), 0, N_DOM * N_RAY)
    counts = counts.at[busiest].set(TILE_CAP)
    return counts.reshape(N_DOM, N_RAY).astype(jnp.int32)


def with_ends(values, rng, least, top_value):
    extent = values.shape
    spot = [jax.random.randint(jax.random.fold_in(rng, axis), (), 0, extent[axis]) for axis in range(len(extent))]
    values = values.at[tuple(spot)].set(least)
    longest = extent.index(max(extent))
    spot[longest] = (spot[longest] + 1) % extent[longest]
    return values.at[tuple(spot)].set(top_value)


def shard_levels(stream_key, extent, cuts, smallest, top_value):
    loudness, own = 1.0, jax.random.fold_in(stream_key, 6)
    for axis_at, shards_of in cuts:
        draws = jnp.exp(jax.random.uniform(jax.random.fold_in(own, axis_at), (shards_of,), jnp.float32, smallest / len(cuts), top_value / len(cuts)))
        loudness = loudness * jnp.repeat(draws, extent[axis_at] // shards_of).reshape([-1 if axis == axis_at else 1 for axis in range(len(extent))])
    return loudness


def bell_draw(rng, extent, spread, reach, pieces=(), kind=jnp.bfloat16):
    drawn = spread * jax.random.normal(rng, extent, jnp.float32)
    if pieces:
        drawn = drawn * shard_levels(rng, extent, pieces, -0.22, 0.18)
    return jnp.clip(drawn, -reach, reach).astype(kind)


def setup_inputs(seed: int = 0) -> dict:
    key_list = jax.random.split(jax.random.key(seed), 10)
    projections = draw_projections(jax.random.fold_in(key_list[9], 71), 0)
    phase_kernel = bell_draw(key_list[1], (2 * HALF + 1,), (2 * HALF + 1) ** -0.5, 0.5)
    image = bell_draw(key_list[2], (PIX, SLICES), 1.0, 6.0, ((0, 8),))
    tile_library = bell_draw(key_list[3], (N_DOM, N_RAY, LIB, TILE, TILE), (TILE * TILE_CAP // N_DOM) ** -0.5, 0.09375, ((0, 8), (1, 4)))
    tile_entry = with_ends(jax.random.randint(key_list[4], (N_DOM, N_RAY, TILE_CAP), 0, LIB), jax.random.fold_in(key_list[4], 1), 0, LIB - 1).astype(jnp.int32)
    tile_image = with_ends(jax.random.randint(key_list[5], (N_DOM, N_RAY, TILE_CAP), 0, IB_DEV), jax.random.fold_in(key_list[5], 1), 0, IB_DEV - 1).astype(jnp.int32)
    tile_slot = with_ends(jax.random.randint(key_list[6], (N_DOM, N_RAY, TILE_CAP), 0, N_DOM), jax.random.fold_in(key_list[6], 1), 0, N_DOM - 1).astype(jnp.int32)
    tile_count = draw_tile_count(jax.random.fold_in(key_list[9], 71), 0)
    slot_block = with_ends(jax.random.randint(key_list[8], (N_DOM, N_RAY, N_DOM), 0, RAY_BLOCKS), jax.random.fold_in(key_list[8], 1), 0, RAY_BLOCKS - 1).astype(jnp.int32)
    return dict(projections=projections, phase_kernel=phase_kernel, image=image, tile_library=tile_library, tile_entry=tile_entry, tile_image=tile_image, tile_slot=tile_slot, tile_count=tile_count, slot_block=slot_block)


relax_factor = 0.25


def toeplitz(kernel, tile_size):
    taps = kernel.shape[0]
    padded = jnp.concatenate([kernel, jnp.zeros((2 * tile_size + 1 - taps,), kernel.dtype)])
    tiled = jnp.tile(padded, tile_size)[: 2 * tile_size * tile_size]
    return tiled.reshape(tile_size, 2 * tile_size).T


def phase_angle(row_block, kernel):
    half_width = (kernel.shape[0] - 1) // 2
    block_count = DET // TILE
    padded = jnp.pad(row_block, ((0, 0), (half_width, 2 * TILE - half_width)))
    blocks = padded.reshape(SLICES, block_count + 2, TILE)
    windows = jnp.concatenate([blocks[:, :block_count], blocks[:, 1:block_count + 1]], axis=-1)
    weights = toeplitz(kernel, TILE).astype(jnp.float32)
    filtered = jnp.einsum("sbi,ij->sbj", windows.astype(jnp.float32), weights)
    return filtered.reshape(SLICES, DET).astype(jnp.bfloat16)


def reference(projections, phase_kernel, image, tile_library, tile_entry, tile_image, tile_slot, tile_count, slot_block):
    phase = lax.map(lambda row_block: phase_angle(row_block, phase_kernel), projections)
    by_slice = jnp.swapaxes(phase, 0, 1)
    profile = lax.map(lambda plane: jnp.median(plane.astype(jnp.float32), axis=0), by_slice)
    padded = jnp.pad(profile, ((0, 0), (SMOOTH, SMOOTH)))
    window_sum = jnp.zeros_like(profile)
    for offset in range(2 * SMOOTH + 1):
        window_sum = window_sum + padded[:, offset:offset + DET]
    position = jnp.arange(DET)
    in_range = (jnp.minimum(position + SMOOTH, DET - 1) - jnp.maximum(position - SMOOTH, 0) + 1).astype(jnp.float32)
    stripe = (profile - window_sum / in_range).astype(jnp.bfloat16)
    corrected = (phase.astype(jnp.float32) - stripe.astype(jnp.float32)[None]).astype(jnp.bfloat16)

    block_count = DET // TILE
    per_owner = DET // (N_RAY * TILE)
    image_blocks = image.reshape(N_DOM, IB_DEV, TILE, SLICES)

    def device_tiles(device_index):
        subdomain = device_index // N_RAY
        quarter = device_index % N_RAY
        library = tile_library[subdomain, quarter]
        entries = tile_entry[subdomain, quarter]
        images = tile_image[subdomain, quarter]
        slots = tile_slot[subdomain, quarter]
        live_mask = jnp.arange(TILE_CAP) < tile_count[subdomain, quarter]
        matrices = library[entries].astype(jnp.float32)
        return subdomain, quarter, matrices, images, slots, live_mask

    def ray_targets(subdomain, quarter):
        carried = slot_block[:, quarter, subdomain]
        angle_index = jnp.arange(N_DOM) * ANG_DEV + carried // per_owner
        column_block = quarter * per_owner + carried % per_owner
        return angle_index, column_block

    def forward_step(device_index, forward):
        subdomain, quarter, matrices, images, slots, live_mask = device_tiles(device_index)
        target = jnp.where(live_mask, slots, N_DOM)
        sources = image_blocks[subdomain][images].astype(jnp.float32)
        product = jnp.einsum("krp,kps->ksr", matrices, sources)
        partial_value = jnp.zeros((N_DOM, SLICES, TILE), jnp.float32).at[target].add(product, mode="drop")
        rounded = lax.optimization_barrier(partial_value.astype(jnp.bfloat16))
        angle_index, column_block = ray_targets(subdomain, quarter)
        return forward.at[angle_index, :, column_block, :].add(rounded.astype(jnp.float32))

    forward = lax.fori_loop(0, N_DOM * N_RAY, forward_step, jnp.zeros((NA, SLICES, block_count, TILE), jnp.float32))
    residual = (corrected.astype(jnp.float32) - forward.reshape(NA, SLICES, DET)).astype(jnp.bfloat16)
    residual_blocks = residual.reshape(NA, SLICES, block_count, TILE)

    def adjoint_step(device_index, gradient):
        subdomain, quarter, matrices, images, slots, live_mask = device_tiles(device_index)
        angle_index, column_block = ray_targets(subdomain, quarter)
        returned = residual_blocks[angle_index, :, column_block, :].astype(jnp.float32)
        image_target = jnp.where(live_mask, images, IB_DEV)
        product = jnp.einsum("krp,ksr->kps", matrices, returned[slots])
        local_sum = jnp.zeros((IB_DEV, TILE, SLICES), jnp.float32).at[image_target].add(product, mode="drop")
        return gradient.at[subdomain].add(local_sum)

    gradient = lax.fori_loop(0, N_DOM * N_RAY, adjoint_step, jnp.zeros((N_DOM, IB_DEV, TILE, SLICES), jnp.float32))
    image_next = image.astype(jnp.float32) + relax_factor * gradient.reshape(PIX, SLICES)
    return residual, image_next
```

```python
import functools

import jax
import jax.numpy as jnp
from jax import lax
from jax.experimental import pallas as pl
from jax.experimental.pallas import tpu as pltpu
from jax.sharding import PartitionSpec as P

SMOOTH = 8


relax_factor = 0.25


def with_halo(cells, sides, width):
    for axis, dim in sides:
        count = lax.axis_size(axis)
        ends = count - 1
        head = lax.slice_in_dim(cells, 0, width, axis=dim)
        tail = lax.slice_in_dim(cells, cells.shape[dim] - width, cells.shape[dim], axis=dim)
        cells = jnp.concatenate(
            [
                lax.ppermute(tail, axis, [(i, (i + 1) % count) for i in range(ends)]),
                cells,
                lax.ppermute(head, axis, [((i + 1) % count, i) for i in range(ends)]),
            ],
            axis=dim,
        )
    return cells


def toeplitz(kernel, tile_size):
    taps = kernel.shape[0]
    padded = jnp.concatenate([kernel, jnp.zeros((2 * tile_size + 1 - taps,), kernel.dtype)])
    tiled = jnp.tile(padded, tile_size)[: 2 * tile_size * tile_size]
    return tiled.reshape(tile_size, 2 * tile_size).T


def phase_filter(projections, phase_kernel, tile_size):
    half_width = (phase_kernel.shape[0] - 1) // 2
    angles, slices, columns = projections.shape
    block_count = columns // tile_size
    rimmed = with_halo(projections, (("ray", 2),), half_width)
    padded = jnp.pad(rimmed, ((0, 0), (0, 0), (0, 2 * tile_size - 2 * half_width)))
    blocks = padded.reshape(angles, slices, block_count + 2, tile_size)
    windows = jnp.concatenate(
        [blocks[:, :, :block_count], blocks[:, :, 1 : block_count + 1]], axis=-1
    )
    filtered = jnp.einsum(
        "asbi,ij->asbj",
        windows,
        toeplitz(phase_kernel, tile_size),
        preferred_element_type=jnp.float32,
    )
    return filtered.reshape(angles, slices, columns).astype(jnp.bfloat16)


def stripe_profile(gathered):
    profile = jnp.median(gathered.astype(jnp.float32), axis=0)
    columns = profile.shape[1]
    rimmed = with_halo(profile, (("ray", 1),), SMOOTH)
    window_sum = jnp.zeros_like(profile)
    for offset in range(2 * SMOOTH + 1):
        window_sum = window_sum + rimmed[:, offset : offset + columns]
    position = lax.axis_index("ray") * columns + jnp.arange(columns)
    detector = lax.axis_size("ray") * columns
    in_range = (
        jnp.minimum(position + SMOOTH, detector - 1) - jnp.maximum(position - SMOOTH, 0) + 1
    ).astype(jnp.float32)
    return (profile - window_sum / in_range).astype(jnp.bfloat16)


def shards(
    projections,
    phase_kernel,
    image,
    tile_library,
    tile_entry,
    tile_image,
    tile_slot,
    tile_count,
    slot_block,
):
    tile_size = tile_library.shape[-1]
    angles, slices, columns = projections.shape
    phase = phase_filter(projections, phase_kernel, tile_size)
    gathered = lax.all_to_all(phase, "dom", split_axis=1, concat_axis=0, tiled=True)
    stripe = stripe_profile(gathered)
    fixed_rows = (gathered.astype(jnp.float32) - stripe.astype(jnp.float32)[None]).astype(
        jnp.bfloat16
    )
    corrected = lax.all_to_all(fixed_rows, "dom", split_axis=0, concat_axis=1, tiled=True)
    owners = lax.axis_size("dom")
    library = tile_library[0, 0]
    entries = tile_entry[0, 0]
    images = tile_image[0, 0]
    slots = tile_slot[0, 0]
    capacity = entries.shape[0]
    block_size = 64
    turn_count = capacity // block_size
    image_blocks = image.reshape(-1, tile_size, slices)
    block_total = image_blocks.shape[0]
    live_mask = jnp.arange(capacity) < tile_count[0, 0]
    slot_target = jnp.where(live_mask, slots, owners)
    image_target = jnp.where(live_mask, images, block_total)

    def forward_turn(turn_index, partial_value):
        first_tile = turn_index * block_size
        chosen = lax.dynamic_slice_in_dim(entries, first_tile, block_size)
        placed = lax.dynamic_slice_in_dim(images, first_tile, block_size)
        destined = lax.dynamic_slice_in_dim(slot_target, first_tile, block_size)
        product = jnp.einsum(
            "krp,kps->ksr",
            library[chosen],
            image_blocks[placed],
            preferred_element_type=jnp.float32,
        )
        return partial_value.at[destined].add(product, mode="drop")

    partial_value = lax.fori_loop(
        0, turn_count, forward_turn, jnp.zeros((owners, slices, tile_size), jnp.float32)
    )
    received = lax.all_to_all(
        partial_value.astype(jnp.bfloat16), "dom", split_axis=0, concat_axis=0, tiled=True
    )
    per_owner = columns // tile_size
    carried = slot_block[0, 0]
    block_ids = jnp.arange(angles * per_owner).reshape(angles, per_owner)
    selector = (block_ids[:, :, None] == carried[None, None, :]).astype(jnp.bfloat16)
    forward = jnp.einsum("abd,dst->asbt", selector, received, preferred_element_type=jnp.float32)
    residual = (corrected.astype(jnp.float32) - forward.reshape(angles, slices, columns)).astype(
        jnp.bfloat16
    )
    back = jnp.einsum(
        "abd,asbt->dst",
        selector,
        residual.reshape(angles, slices, per_owner, tile_size),
        preferred_element_type=jnp.float32,
    ).astype(jnp.bfloat16)
    returned = lax.all_to_all(back, "dom", split_axis=0, concat_axis=0, tiled=True)

    def adjoint_turn(turn_index, gradient):
        first_tile = turn_index * block_size
        chosen = lax.dynamic_slice_in_dim(entries, first_tile, block_size)
        sourced = lax.dynamic_slice_in_dim(slots, first_tile, block_size)
        destined = lax.dynamic_slice_in_dim(image_target, first_tile, block_size)
        product = jnp.einsum(
            "krp,ksr->kps", library[chosen], returned[sourced], preferred_element_type=jnp.float32
        )
        return gradient.at[destined].add(product, mode="drop")

    gradient = lax.fori_loop(
        0, turn_count, adjoint_turn, jnp.zeros((block_total, tile_size, slices), jnp.float32)
    )
    gradient = gradient.reshape(-1, slices)
    rows_own = gradient.shape[0] // lax.axis_size("ray")
    update = lax.psum_scatter(gradient, "ray", scatter_dimension=0, tiled=True)
    own_image = lax.dynamic_slice_in_dim(image, lax.axis_index("ray") * rows_own, rows_own)
    image_next = own_image.astype(jnp.float32) + relax_factor * update
    return (residual, image_next)


MESH = pl.DeviceIdType.MESH
NT = (((1,), (1,)), ((), ()))
NN = (((1,), (0,)), ((), ()))


def dot(a, b, dims):
    return lax.dot_general(a, b, dims, preferred_element_type=jnp.float32)


def sort_pairs(count):
    p = 1
    while p < count:
        k = p
        while k >= 1:
            for j in range(k % p, count - k, 2 * k):
                for i in range(min(k, count - j - k)):
                    if (i + j) // (2 * p) == (i + j + k) // (2 * p):
                        yield i + j, i + j + k
            k //= 2
        p *= 2


def step_kernel(
    owners,
    quarters,
    taps_ref,
    proj_ref,
    image_ref,
    library_ref,
    entry_ref,
    place_ref,
    slot_ref,
    count_ref,
    carried_ref,
    residual_ref,
    update_ref,
    rim,
    phase_out,
    phase_in,
    shifted,
    mixed,
    partial_rows,
    partial_out,
    partial_in,
    stripes,
    forward,
    blocks,
    back_out,
    back_in,
    back_rows,
    update_rows,
    update_out,
    update_in,
    halo_send,
    halo_recv,
    phase_send,
    phase_recv,
    stripe_send,
    stripe_recv,
    partial_send,
    partial_recv,
    back_send,
    back_recv,
    update_send,
    update_recv,
):
    f32, bf16 = jnp.float32, jnp.bfloat16
    me, ray = lax.axis_index("dom"), lax.axis_index("ray")
    slices, columns = proj_ref.shape
    tile = library_ref.shape[-1]
    entries = library_ref.shape[0]
    places = image_ref.shape[1]
    count = columns // tile
    per = slices // owners
    half = tile // 2
    own_places = places // quarters

    def dom_peer(k):
        return lax.rem(me + k, owners)

    def ray_peer(k):
        return lax.rem(ray + k, quarters)

    barrier = pltpu.get_barrier_semaphore()
    for k in range(1, owners):
        pl.semaphore_signal(barrier, inc=1, device_id=(dom_peer(k), ray), device_id_type=MESH)
    for k in range(1, quarters):
        pl.semaphore_signal(barrier, inc=1, device_id=(me, ray_peer(k)), device_id_type=MESH)

    def dom_copy(src, dst, send, recv, k):
        return pltpu.make_async_remote_copy(
            src_ref=src,
            dst_ref=dst,
            send_sem=send.at[k],
            recv_sem=recv.at[k],
            device_id=(dom_peer(k), ray),
            device_id_type=MESH,
        )

    def ray_copy(src, dst, send, recv, slot, k):
        return pltpu.make_async_remote_copy(
            src_ref=src,
            dst_ref=dst,
            send_sem=send.at[slot],
            recv_sem=recv.at[slot],
            device_id=(me, ray_peer(k)),
            device_id_type=MESH,
        )

    for b in range(count):
        rim[b + 1] = proj_ref[:, b * tile : (b + 1) * tile]
    spread = jnp.broadcast_to(taps_ref[...], (tile, 2 * tile))
    weights = pltpu.roll(spread, 0, 1, stride=1, stride_axis=0).astype(bf16)

    pl.semaphore_wait(barrier, owners + quarters - 2)

    halos = [
        ray_copy(
            proj_ref.at[:, pl.ds(columns - tile, tile)], rim.at[0], halo_send, halo_recv, 0, 1
        ),
        ray_copy(
            proj_ref.at[:, pl.ds(0, tile)],
            rim.at[count + 1],
            halo_send,
            halo_recv,
            1,
            quarters - 1,
        ),
    ]
    for copy in halos:
        copy.start()

    capacity = entry_ref.shape[1]
    slot = slot_ref[...]
    relative = jnp.where(slot >= me, slot - me, slot - me + owners)
    alive = lax.broadcasted_iota(jnp.int32, (1, capacity), 1) < count_ref[0, 0]
    code = jnp.where(alive, entry_ref[...] * owners + relative, -1)
    pick = jnp.where(
        lax.broadcasted_iota(jnp.int32, (entries * owners, capacity), 0) == code, 1.0, 0.0
    ).astype(bf16)
    where_to = jnp.where(
        lax.broadcasted_iota(jnp.int32, (places, capacity), 0) == place_ref[...], 1.0, 0.0
    ).astype(bf16)
    uses = dot(pick, where_to, NT).astype(bf16)
    uses_back = dot(where_to, pick, NT).astype(bf16)

    for copy in halos:
        copy.wait()

    @pl.when(ray == 0)
    def _():
        rim[0] = jnp.zeros((slices, tile), bf16)

    @pl.when(ray == quarters - 1)
    def _():
        rim[count + 1] = jnp.zeros((slices, tile), bf16)

    rows = (count + 1) * slices
    phase = dot(rim[0 : count + 1].reshape(rows, tile), weights[:, :tile], NT)
    phase = phase + dot(rim[1 : count + 2].reshape(rows, tile), weights[:, tile:], NT)
    phase = phase.astype(bf16).astype(f32)
    grouped = phase.reshape(count + 1, owners, per, tile)
    for owner in range(owners):
        phase_out[owner] = grouped[:, owner].astype(bf16)
    phase_in[0] = phase_out[me]
    phases = [
        dom_copy(phase_out.at[dom_peer(k)], phase_in.at[k], phase_send, phase_recv, k)
        for k in range(1, owners)
    ]
    for copy in phases:
        copy.start()

    turned = pltpu.roll(phase, half, 1).reshape(count + 1, slices, tile)
    lane = lax.broadcasted_iota(jnp.int32, (1, 1, tile), 2)
    shifted[...] = jnp.where(lane < half, turned[:count], turned[1:])

    group = 8

    def mix(step, carry):
        for inner in range(group):
            s = step * group + inner
            mixed[s] = dot(uses, image_ref[s], NN).reshape(entries, owners, tile)
        return carry

    lax.fori_loop(0, slices // group, mix, 0)

    total = jnp.zeros((slices * owners, tile), f32)
    for entry in range(0, entries, 2):
        left = jnp.concatenate(
            [
                mixed[:, entry].reshape(slices * owners, tile).astype(bf16),
                mixed[:, entry + 1].reshape(slices * owners, tile).astype(bf16),
            ],
            axis=1,
        )
        right = jnp.concatenate([library_ref[entry], library_ref[entry + 1]], axis=1)
        total = total + dot(left, right, NT)
    partial_rows[...] = total
    for k in range(1, owners):
        partial_out[k] = partial_rows[pl.ds(k, slices, stride=owners), :].astype(bf16)
    partial_in[me] = partial_rows[pl.ds(0, slices, stride=owners), :].astype(bf16)
    partials = [
        dom_copy(partial_out.at[k], partial_in.at[me], partial_send, partial_recv, k)
        for k in range(1, owners)
    ]

    for copy in phases:
        copy.wait_recv()

    values = [phase_in[a].astype(f32) for a in range(owners)]
    for i, j in sort_pairs(owners):
        values[i], values[j] = jnp.minimum(values[i], values[j]), jnp.maximum(values[i], values[j])
    middle = (values[owners // 2 - 1] + values[owners // 2]) * 0.5
    profile = jnp.concatenate([middle[b] for b in range(count + 1)], axis=1)
    width = columns + tile
    detector = quarters * columns
    position = ray * columns - half + lax.broadcasted_iota(jnp.int32, (1, width), 1)
    profile = jnp.where((position >= 0) & (position < detector), profile, 0.0)
    run = profile
    reach = 1
    while reach < 2 * SMOOTH:
        run = run + pltpu.roll(run, reach, 1)
        reach *= 2
    window = pltpu.roll(run, width - (SMOOTH - 1), 1) + pltpu.roll(profile, width - SMOOTH, 1)
    in_range = (
        jnp.minimum(position + SMOOTH, detector - 1) - jnp.maximum(position - SMOOTH, 0) + 1
    ).astype(f32)
    stripe = pltpu.roll(profile - window / in_range, width - half, 1)
    for b in range(count):
        stripes[me, b] = stripe[:, b * tile : (b + 1) * tile].astype(bf16)
    spreads = [
        dom_copy(stripes.at[me], stripes.at[me], stripe_send, stripe_recv, k)
        for k in range(1, owners)
    ]
    for copy in spreads:
        copy.start()
    for copy in partials:
        copy.start()

    for copy in partials:
        copy.wait_recv()

    def project(b, carry):
        total = jnp.zeros((slices, tile), f32)
        for d in range(owners):
            share = jnp.where(carried_ref[0, d] == b, 1.0, 0.0).astype(f32)
            total = total + share * partial_in[d].astype(f32)
        forward[b] = total
        return carry

    lax.fori_loop(0, count, project, 0)

    for copy in spreads:
        copy.wait_recv()

    for b in range(count):
        stripe_all = jnp.concatenate([stripes[o, b].astype(f32) for o in range(owners)], axis=0)
        corrected = (shifted[b] - stripe_all).astype(bf16).astype(f32)
        rest = (corrected - forward[b]).astype(bf16)
        blocks[b] = rest
        residual_ref[:, b * tile : (b + 1) * tile] = rest

    for k in range(1, owners):
        back_out[k] = blocks[carried_ref[0, dom_peer(k)]]
    backs = [
        dom_copy(back_out.at[k], back_in.at[owners - k], back_send, back_recv, k)
        for k in range(1, owners)
    ]
    for copy in backs:
        copy.start()
    back_in[0] = blocks[carried_ref[0, me]]
    for copy in backs:
        copy.wait_recv()

    for k in range(owners):
        back_rows[pl.ds(k, slices, stride=owners), :] = back_in[k].astype(f32)
    gathered = back_rows[...].astype(bf16)
    for entry in range(entries):
        mixed[:, entry] = dot(gathered, library_ref[entry], NN).reshape(slices, owners, tile)

    def unmix(step, carry):
        for inner in range(group):
            s = step * group + inner
            piece = mixed[s].reshape(entries * owners, tile).astype(bf16)
            start = pl.multiple_of(s * places, places)
            update_rows[pl.ds(start, places), :] = dot(uses_back, piece, NN)
        return carry

    lax.fori_loop(0, slices // group, unmix, 0)
    for place in range(places):
        update_out[place // own_places, place % own_places] = update_rows[
            pl.ds(place, slices, stride=places), :
        ].astype(bf16)
    updates = [
        ray_copy(
            update_out.at[ray_peer(k)], update_in.at[k], update_send, update_recv, k, k
        )
        for k in range(1, quarters)
    ]
    for copy in updates:
        copy.start()
    for copy in updates:
        copy.wait_recv()
    for place in range(own_places):
        amount = update_out[ray, place].astype(f32)
        for k in range(1, quarters):
            amount = amount + update_in[k, place].astype(f32)
        update_ref[place * tile : (place + 1) * tile, :] = amount.T
    for copy in phases + partials + spreads + backs + updates:
        copy.wait_send()


def fast_shards(
    projections,
    phase_kernel,
    image,
    tile_library,
    tile_entry,
    tile_image,
    tile_slot,
    tile_count,
    slot_block,
):
    f32, bf16 = jnp.float32, jnp.bfloat16
    owners, quarters = lax.axis_size("dom"), lax.axis_size("ray")
    entries, tile = tile_library.shape[2], tile_library.shape[-1]
    _, slices, columns = projections.shape
    count = columns // tile
    places = image.shape[0] // tile
    per = slices // owners
    own_places = places // quarters
    taps = jnp.pad(phase_kernel.astype(f32), (0, 2 * tile - phase_kernel.shape[0]))[None]
    by_slice = image.reshape(places, tile, slices).transpose(2, 0, 1)
    vmem = pl.BlockSpec(memory_space=pltpu.VMEM)
    smem = pl.BlockSpec(memory_space=pltpu.SMEM)
    sems = pltpu.SemaphoreType.DMA
    residual, update = pl.pallas_call(
        functools.partial(step_kernel, owners, quarters),
        out_shape=(
            jax.ShapeDtypeStruct((slices, columns), bf16),
            jax.ShapeDtypeStruct((own_places * tile, slices), f32),
        ),
        in_specs=[vmem] * 7 + [smem] * 2,
        out_specs=(vmem, vmem),
        scratch_shapes=[
            pltpu.VMEM((count + 2, slices, tile), bf16),
            pltpu.VMEM((owners, count + 1, per, tile), bf16),
            pltpu.VMEM((owners, count + 1, per, tile), bf16),
            pltpu.VMEM((count, slices, tile), f32),
            pltpu.VMEM((slices, entries, owners, tile), f32),
            pltpu.VMEM((slices * owners, tile), f32),
            pltpu.VMEM((owners, slices, tile), bf16),
            pltpu.VMEM((owners, slices, tile), bf16),
            pltpu.VMEM((owners, count, per, tile), bf16),
            pltpu.VMEM((count, slices, tile), f32),
            pltpu.VMEM((count, slices, tile), bf16),
            pltpu.VMEM((owners, slices, tile), bf16),
            pltpu.VMEM((owners, slices, tile), bf16),
            pltpu.VMEM((slices * owners, tile), f32),
            pltpu.VMEM((slices * places, tile), f32),
            pltpu.VMEM((quarters, own_places, slices, tile), bf16),
            pltpu.VMEM((quarters, own_places, slices, tile), bf16),
            sems((2,)),
            sems((2,)),
            sems((owners,)),
            sems((owners,)),
            sems((owners,)),
            sems((owners,)),
            sems((owners,)),
            sems((owners,)),
            sems((owners,)),
            sems((owners,)),
            sems((quarters,)),
            sems((quarters,)),
        ],
        compiler_params=pltpu.CompilerParams(
            collective_id=0, has_side_effects=True, vmem_limit_bytes=48 * 1024 * 1024
        ),
    )(
        taps,
        projections[0],
        by_slice,
        tile_library[0, 0],
        tile_entry[0],
        tile_image[0],
        tile_slot[0],
        tile_count,
        slot_block[0],
    )
    rows_own = own_places * tile
    own_image = lax.dynamic_slice_in_dim(image, lax.axis_index("ray") * rows_own, rows_own)
    return residual[None], own_image.astype(f32) + relax_factor * update


def fits_kernel(projections, phase_kernel, image, tile_library, tile_entry, *rest):
    owners, quarters = lax.axis_size("dom"), lax.axis_size("ray")
    tile = tile_library.shape[-1]
    angles, slices, columns = projections.shape
    return (
        angles == 1
        and slices % 16 == 0
        and slices == 8 * owners
        and owners == 8
        and tile == 128
        and phase_kernel.shape[0] == tile + 1
        and columns % tile == 0
        and tile_library.shape[2] % 2 == 0
        and (image.shape[0] // tile) % (16 * 1) == 0
        and (image.shape[0] // tile) % quarters == 0
        and tile_entry.shape[2] <= 256
    )


def any_shards(*args):
    if fits_kernel(*args):
        return fast_shards(*args)
    return shards(*args)


def solution(mesh):
    return jax.shard_map(
        any_shards,
        mesh=mesh,
        in_specs=(
            P("dom", None, "ray"),
            P(),
            P("dom", None),
            P("dom", "ray", None, None, None),
            P("dom", "ray", None),
            P("dom", "ray", None),
            P("dom", "ray", None),
            P("dom", "ray"),
            P("dom", "ray", None),
        ),
        out_specs=(P("dom", None, "ray"), P(("dom", "ray"), None)),
        check_vma=False,
    )
```

```python
import functools

import jax
import jax.numpy as jnp
from jax import lax
from jax.experimental import pallas as pl
from jax.experimental.pallas import tpu as pltpu
from jax.sharding import PartitionSpec as P

SMOOTH = 8


relax_factor = 0.25


def with_halo(cells, sides, width):
    for axis, dim in sides:
        count = lax.axis_size(axis)
        ends = count - 1
        head = lax.slice_in_dim(cells, 0, width, axis=dim)
        tail = lax.slice_in_dim(cells, cells.shape[dim] - width, cells.shape[dim], axis=dim)
        cells = jnp.concatenate(
            [
                lax.ppermute(tail, axis, [(i, (i + 1) % count) for i in range(ends)]),
                cells,
                lax.ppermute(head, axis, [((i + 1) % count, i) for i in range(ends)]),
            ],
            axis=dim,
        )
    return cells


def toeplitz(kernel, tile_size):
    taps = kernel.shape[0]
    padded = jnp.concatenate([kernel, jnp.zeros((2 * tile_size + 1 - taps,), kernel.dtype)])
    tiled = jnp.tile(padded, tile_size)[: 2 * tile_size * tile_size]
    return tiled.reshape(tile_size, 2 * tile_size).T


def phase_filter(projections, phase_kernel, tile_size):
    half_width = (phase_kernel.shape[0] - 1) // 2
    angles, slices, columns = projections.shape
    block_count = columns // tile_size
    rimmed = with_halo(projections, (("ray", 2),), half_width)
    padded = jnp.pad(rimmed, ((0, 0), (0, 0), (0, 2 * tile_size - 2 * half_width)))
    blocks = padded.reshape(angles, slices, block_count + 2, tile_size)
    windows = jnp.concatenate(
        [blocks[:, :, :block_count], blocks[:, :, 1 : block_count + 1]], axis=-1
    )
    filtered = jnp.einsum(
        "asbi,ij->asbj",
        windows,
        toeplitz(phase_kernel, tile_size),
        preferred_element_type=jnp.float32,
    )
    return filtered.reshape(angles, slices, columns).astype(jnp.bfloat16)


def stripe_profile(gathered):
    profile = jnp.median(gathered.astype(jnp.float32), axis=0)
    columns = profile.shape[1]
    rimmed = with_halo(profile, (("ray", 1),), SMOOTH)
    window_sum = jnp.zeros_like(profile)
    for offset in range(2 * SMOOTH + 1):
        window_sum = window_sum + rimmed[:, offset : offset + columns]
    position = lax.axis_index("ray") * columns + jnp.arange(columns)
    detector = lax.axis_size("ray") * columns
    in_range = (
        jnp.minimum(position + SMOOTH, detector - 1) - jnp.maximum(position - SMOOTH, 0) + 1
    ).astype(jnp.float32)
    return (profile - window_sum / in_range).astype(jnp.bfloat16)


def shards(
    projections,
    phase_kernel,
    image,
    tile_library,
    tile_entry,
    tile_image,
    tile_slot,
    tile_count,
    slot_block,
):
    tile_size = tile_library.shape[-1]
    angles, slices, columns = projections.shape
    phase = phase_filter(projections, phase_kernel, tile_size)
    gathered = lax.all_to_all(phase, "dom", split_axis=1, concat_axis=0, tiled=True)
    stripe = stripe_profile(gathered)
    fixed_rows = (gathered.astype(jnp.float32) - stripe.astype(jnp.float32)[None]).astype(
        jnp.bfloat16
    )
    corrected = lax.all_to_all(fixed_rows, "dom", split_axis=0, concat_axis=1, tiled=True)
    owners = lax.axis_size("dom")
    library = tile_library[0, 0]
    entries = tile_entry[0, 0]
    images = tile_image[0, 0]
    slots = tile_slot[0, 0]
    capacity = entries.shape[0]
    block_size = 64
    turn_count = capacity // block_size
    image_blocks = image.reshape(-1, tile_size, slices)
    block_total = image_blocks.shape[0]
    live_mask = jnp.arange(capacity) < tile_count[0, 0]
    slot_target = jnp.where(live_mask, slots, owners)
    image_target = jnp.where(live_mask, images, block_total)

    def forward_turn(turn_index, partial_value):
        first_tile = turn_index * block_size
        chosen = lax.dynamic_slice_in_dim(entries, first_tile, block_size)
        placed = lax.dynamic_slice_in_dim(images, first_tile, block_size)
        destined = lax.dynamic_slice_in_dim(slot_target, first_tile, block_size)
        product = jnp.einsum(
            "krp,kps->ksr",
            library[chosen],
            image_blocks[placed],
            preferred_element_type=jnp.float32,
        )
        return partial_value.at[destined].add(product, mode="drop")

    partial_value = lax.fori_loop(
        0, turn_count, forward_turn, jnp.zeros((owners, slices, tile_size), jnp.float32)
    )
    received = lax.all_to_all(
        partial_value.astype(jnp.bfloat16), "dom", split_axis=0, concat_axis=0, tiled=True
    )
    per_owner = columns // tile_size
    carried = slot_block[0, 0]
    block_ids = jnp.arange(angles * per_owner).reshape(angles, per_owner)
    selector = (block_ids[:, :, None] == carried[None, None, :]).astype(jnp.bfloat16)
    forward = jnp.einsum("abd,dst->asbt", selector, received, preferred_element_type=jnp.float32)
    residual = (corrected.astype(jnp.float32) - forward.reshape(angles, slices, columns)).astype(
        jnp.bfloat16
    )
    back = jnp.einsum(
        "abd,asbt->dst",
        selector,
        residual.reshape(angles, slices, per_owner, tile_size),
        preferred_element_type=jnp.float32,
    ).astype(jnp.bfloat16)
    returned = lax.all_to_all(back, "dom", split_axis=0, concat_axis=0, tiled=True)

    def adjoint_turn(turn_index, gradient):
        first_tile = turn_index * block_size
        chosen = lax.dynamic_slice_in_dim(entries, first_tile, block_size)
        sourced = lax.dynamic_slice_in_dim(slots, first_tile, block_size)
        destined = lax.dynamic_slice_in_dim(image_target, first_tile, block_size)
        product = jnp.einsum(
            "krp,ksr->kps", library[chosen], returned[sourced], preferred_element_type=jnp.float32
        )
        return gradient.at[destined].add(product, mode="drop")

    gradient = lax.fori_loop(
        0, turn_count, adjoint_turn, jnp.zeros((block_total, tile_size, slices), jnp.float32)
    )
    gradient = gradient.reshape(-1, slices)
    rows_own = gradient.shape[0] // lax.axis_size("ray")
    update = lax.psum_scatter(gradient, "ray", scatter_dimension=0, tiled=True)
    own_image = lax.dynamic_slice_in_dim(image, lax.axis_index("ray") * rows_own, rows_own)
    image_next = own_image.astype(jnp.float32) + relax_factor * update
    return (residual, image_next)


MESH = pl.DeviceIdType.MESH
NT = (((1,), (1,)), ((), ()))
NN = (((1,), (0,)), ((), ()))


def dot(a, b, dims):
    return lax.dot_general(a, b, dims, preferred_element_type=jnp.float32)


def sort_pairs(count):
    p = 1
    while p < count:
        k = p
        while k >= 1:
            for j in range(k % p, count - k, 2 * k):
                for i in range(min(k, count - j - k)):
                    if (i + j) // (2 * p) == (i + j + k) // (2 * p):
                        yield i + j, i + j + k
            k //= 2
        p *= 2


def step_kernel(
    owners,
    quarters,
    taps_ref,
    proj_any,
    image_any,
    library_any,
    entry_ref,
    place_ref,
    slot_ref,
    count_ref,
    carried_ref,
    residual_ref,
    next_ref,
    rim,
    phase_out,
    phase_in,
    shifted,
    mixed,
    partial_rows,
    partial_out,
    partial_in,
    stripes,
    forward,
    blocks,
    back_out,
    back_in,
    back_rows,
    update_rows,
    update_out,
    update_in,
    halo_send,
    halo_recv,
    phase_send,
    phase_recv,
    stripe_send,
    stripe_recv,
    partial_send,
    partial_recv,
    back_send,
    back_recv,
    update_send,
    update_recv,
    taps_wide,
    proj_ref,
    image_rows,
    image_ref,
    library_ref,
    load_sem,
):
    f32, bf16 = jnp.float32, jnp.bfloat16
    me, ray = lax.axis_index("dom"), lax.axis_index("ray")
    slices, columns = proj_ref.shape
    tile = library_ref.shape[-1]
    entries = library_ref.shape[0]
    places = image_rows.shape[0] // tile
    count = columns // tile
    per = slices // owners
    half = tile // 2
    own_places = places // quarters

    def dom_peer(k):
        return lax.rem(me + k, owners)

    def ray_peer(k):
        return lax.rem(ray + k, quarters)

    loads = [
        pltpu.make_async_copy(proj_any.at[0], proj_ref, load_sem.at[0]),
        pltpu.make_async_copy(image_any, image_rows, load_sem.at[1]),
        pltpu.make_async_copy(library_any.at[0, 0], library_ref, load_sem.at[2]),
    ]
    for copy in loads:
        copy.start()

    barrier = pltpu.get_barrier_semaphore()
    for k in range(1, owners):
        pl.semaphore_signal(barrier, inc=1, device_id=(dom_peer(k), ray), device_id_type=MESH)
    for k in range(1, quarters):
        pl.semaphore_signal(barrier, inc=1, device_id=(me, ray_peer(k)), device_id_type=MESH)

    def dom_copy(src, dst, send, recv, k):
        return pltpu.make_async_remote_copy(
            src_ref=src,
            dst_ref=dst,
            send_sem=send.at[k],
            recv_sem=recv.at[k],
            device_id=(dom_peer(k), ray),
            device_id_type=MESH,
        )

    def ray_copy(src, dst, send, recv, slot, k):
        return pltpu.make_async_remote_copy(
            src_ref=src,
            dst_ref=dst,
            send_sem=send.at[slot],
            recv_sem=recv.at[slot],
            device_id=(me, ray_peer(k)),
            device_id_type=MESH,
        )

    taps_wide[...] = jnp.zeros((1, 2 * tile), f32)
    taps_wide[:, : taps_ref.shape[1]] = taps_ref[...].astype(f32)
    spread = jnp.broadcast_to(taps_wide[...], (tile, 2 * tile))
    weights = pltpu.roll(spread, 0, 1, stride=1, stride_axis=0).astype(bf16)

    loads[0].wait()
    pl.semaphore_wait(barrier, owners + quarters - 2)

    halos = [
        ray_copy(
            proj_ref.at[:, pl.ds(columns - tile, tile)], rim.at[0], halo_send, halo_recv, 0, 1
        ),
        ray_copy(
            proj_ref.at[:, pl.ds(0, tile)],
            rim.at[count + 1],
            halo_send,
            halo_recv,
            1,
            quarters - 1,
        ),
    ]
    for copy in halos:
        copy.start()

    capacity = entry_ref.shape[1]
    slot = slot_ref[...]
    relative = jnp.where(slot >= me, slot - me, slot - me + owners)
    alive = lax.broadcasted_iota(jnp.int32, (1, capacity), 1) < count_ref[0, 0]
    code = jnp.where(alive, entry_ref[...] * owners + relative, -1)
    pick = jnp.where(
        lax.broadcasted_iota(jnp.int32, (entries * owners, capacity), 0) == code, 1.0, 0.0
    ).astype(bf16)
    where_to = jnp.where(
        lax.broadcasted_iota(jnp.int32, (places, capacity), 0) == place_ref[...], 1.0, 0.0
    ).astype(bf16)
    uses = dot(pick, where_to, NT).astype(bf16)
    uses_back = dot(where_to, pick, NT).astype(bf16)

    for b in range(count):
        rim[b + 1] = proj_ref[:, b * tile : (b + 1) * tile]
    loads[1].wait()
    for place in range(places):
        image_ref[pl.ds(place, slices, stride=places), :] = (
            image_rows[place * tile : (place + 1) * tile, :].astype(f32).T
        )

    group = 8

    def mix(step, carry):
        for inner in range(group):
            s = step * group + inner
            start = pl.multiple_of(s * places, places)
            piece = image_ref[pl.ds(start, places), :].astype(bf16)
            mixed[s] = dot(uses, piece, NN).reshape(entries, owners, tile)
        return carry

    lax.fori_loop(0, slices // group, mix, 0)

    loads[2].wait()
    total = jnp.zeros((slices * owners, tile), f32)
    for entry in range(0, entries, 2):
        left = jnp.concatenate(
            [
                mixed[:, entry].reshape(slices * owners, tile).astype(bf16),
                mixed[:, entry + 1].reshape(slices * owners, tile).astype(bf16),
            ],
            axis=1,
        )
        right = jnp.concatenate([library_ref[entry], library_ref[entry + 1]], axis=1)
        total = total + dot(left, right, NT)
    partial_rows[...] = total
    for k in range(1, owners):
        partial_out[k] = partial_rows[pl.ds(k, slices, stride=owners), :].astype(bf16)
    partial_in[me] = partial_rows[pl.ds(0, slices, stride=owners), :].astype(bf16)
    partials = [
        dom_copy(partial_out.at[k], partial_in.at[me], partial_send, partial_recv, k)
        for k in range(1, owners)
    ]
    for copy in partials:
        copy.start()

    for copy in halos:
        copy.wait()

    @pl.when(ray == 0)
    def _():
        rim[0] = jnp.zeros((slices, tile), bf16)

    @pl.when(ray == quarters - 1)
    def _():
        rim[count + 1] = jnp.zeros((slices, tile), bf16)

    rows = (count + 1) * slices
    phase = dot(rim[0 : count + 1].reshape(rows, tile), weights[:, :tile], NT)
    phase = phase + dot(rim[1 : count + 2].reshape(rows, tile), weights[:, tile:], NT)
    phase = phase.astype(bf16).astype(f32)
    grouped = phase.reshape(count + 1, owners, per, tile)
    for owner in range(owners):
        phase_out[owner] = grouped[:, owner].astype(bf16)
    phase_in[0] = phase_out[me]
    phases = [
        dom_copy(phase_out.at[dom_peer(k)], phase_in.at[k], phase_send, phase_recv, k)
        for k in range(1, owners)
    ]
    for copy in phases:
        copy.start()

    turned = pltpu.roll(phase, half, 1).reshape(count + 1, slices, tile)
    lane = lax.broadcasted_iota(jnp.int32, (1, 1, tile), 2)
    shifted[...] = jnp.where(lane < half, turned[:count], turned[1:])

    for copy in phases:
        copy.wait_recv()

    values = [phase_in[a].astype(f32) for a in range(owners)]
    for i, j in sort_pairs(owners):
        values[i], values[j] = jnp.minimum(values[i], values[j]), jnp.maximum(values[i], values[j])
    middle = (values[owners // 2 - 1] + values[owners // 2]) * 0.5
    profile = jnp.concatenate([middle[b] for b in range(count + 1)], axis=1)
    width = columns + tile
    detector = quarters * columns
    position = ray * columns - half + lax.broadcasted_iota(jnp.int32, (1, width), 1)
    profile = jnp.where((position >= 0) & (position < detector), profile, 0.0)
    run = profile
    reach = 1
    while reach < 2 * SMOOTH:
        run = run + pltpu.roll(run, reach, 1)
        reach *= 2
    window = pltpu.roll(run, width - (SMOOTH - 1), 1) + pltpu.roll(profile, width - SMOOTH, 1)
    in_range = (
        jnp.minimum(position + SMOOTH, detector - 1) - jnp.maximum(position - SMOOTH, 0) + 1
    ).astype(f32)
    stripe = pltpu.roll(profile - window / in_range, width - half, 1)
    for b in range(count):
        stripes[me, b] = stripe[:, b * tile : (b + 1) * tile].astype(bf16)
    steps = owners // 2
    beside = 1 - 2 * lax.rem(me, 2)

    def stripe_copy(source, k, slot):
        return pltpu.make_async_remote_copy(
            src_ref=stripes.at[source],
            dst_ref=stripes.at[source],
            send_sem=stripe_send.at[slot],
            recv_sem=stripe_recv.at[slot],
            device_id=(lax.rem(me + k + owners, owners), ray),
            device_id_type=MESH,
        )

    spreads = [stripe_copy(me, 2 * k, k) for k in range(1, steps)]
    spreads = spreads + [stripe_copy(me, beside, 0)]
    for copy in spreads:
        copy.start()

    for copy in partials:
        copy.wait_recv()

    def project(b, carry):
        total = jnp.zeros((slices, tile), f32)
        for d in range(owners):
            share = jnp.where(carried_ref[0, d] == b, 1.0, 0.0).astype(f32)
            total = total + share * partial_in[d].astype(f32)
        forward[b] = total
        return carry

    lax.fori_loop(0, count, project, 0)

    spreads[-1].wait_recv()
    relays = []
    for k in range(1, steps):
        spreads[k - 1].wait_recv()
        relays.append(stripe_copy(lax.rem(me - 2 * k + owners, owners), beside, steps + k))
        relays[-1].start()
    for copy in relays:
        copy.wait_recv()

    for b in range(count):
        stripe_all = jnp.concatenate([stripes[o, b].astype(f32) for o in range(owners)], axis=0)
        corrected = (shifted[b] - stripe_all).astype(bf16).astype(f32)
        rest = (corrected - forward[b]).astype(bf16)
        blocks[b] = rest
        residual_ref[:, b * tile : (b + 1) * tile] = rest

    for k in range(1, owners):
        back_out[k] = blocks[carried_ref[0, dom_peer(k)]]
    backs = [
        dom_copy(back_out.at[k], back_in.at[owners - k], back_send, back_recv, k)
        for k in range(1, owners)
    ]
    for copy in backs:
        copy.start()
    back_in[0] = blocks[carried_ref[0, me]]
    for copy in backs:
        copy.wait_recv()

    for k in range(owners):
        back_rows[pl.ds(k, slices, stride=owners), :] = back_in[k].astype(f32)
    parts = update_out.shape[0]
    part = slices // parts
    updates = []
    for turn in range(parts):
        rows = part * owners
        gathered = back_rows[turn * rows : (turn + 1) * rows, :].astype(bf16)
        first = turn * part
        for entry in range(entries):
            mixed[first : first + part, entry] = dot(gathered, library_ref[entry], NN).reshape(
                part, owners, tile
            )

        def unmix(step, carry, first=first):
            for inner in range(group):
                s = first + step * group + inner
                piece = mixed[s].reshape(entries * owners, tile).astype(bf16)
                start = pl.multiple_of(s * places, places)
                update_rows[pl.ds(start, places), :] = dot(uses_back, piece, NN)
            return carry

        lax.fori_loop(0, part // group, unmix, 0)
        for place in range(places):
            update_out[turn, place // own_places, place % own_places] = update_rows[
                pl.ds(first * places + place, part, stride=places), :
            ].astype(bf16)
        sent = [
            ray_copy(
                update_out.at[turn, ray_peer(k)],
                update_in.at[turn, k],
                update_send,
                update_recv,
                turn * quarters + k,
                k,
            )
            for k in range(1, quarters)
        ]
        for copy in sent:
            copy.start()
        updates = updates + sent
    for copy in updates:
        copy.wait_recv()
    for place in range(own_places):
        amounts = []
        for turn in range(parts):
            amount = update_out[turn, ray, place].astype(f32)
            for k in range(1, quarters):
                amount = amount + update_in[turn, k, place].astype(f32)
            amounts.append(amount)
        update = jnp.concatenate(amounts, axis=0).T
        start = pl.multiple_of((ray * own_places + place) * tile, tile)
        held = image_rows[pl.ds(start, tile), :].astype(f32)
        next_ref[place * tile : (place + 1) * tile, :] = held + relax_factor * update
    for copy in phases + partials + spreads + relays + backs + updates:
        copy.wait_send()


def fast_shards(
    projections,
    phase_kernel,
    image,
    tile_library,
    tile_entry,
    tile_image,
    tile_slot,
    tile_count,
    slot_block,
):
    f32, bf16 = jnp.float32, jnp.bfloat16
    owners, quarters = lax.axis_size("dom"), lax.axis_size("ray")
    entries, tile = tile_library.shape[2], tile_library.shape[-1]
    _, slices, columns = projections.shape
    count = columns // tile
    places = image.shape[0] // tile
    per = slices // owners
    own_places = places // quarters
    parts = 2
    hbm = pl.BlockSpec(memory_space=pl.ANY)
    vmem = pl.BlockSpec(memory_space=pltpu.VMEM)
    smem = pl.BlockSpec(memory_space=pltpu.SMEM)
    sems = pltpu.SemaphoreType.DMA
    residual, image_next = pl.pallas_call(
        functools.partial(step_kernel, owners, quarters),
        out_shape=(
            jax.ShapeDtypeStruct((slices, columns), bf16),
            jax.ShapeDtypeStruct((own_places * tile, slices), f32),
        ),
        in_specs=[vmem] + [hbm] * 3 + [vmem] * 3 + [smem] * 2,
        out_specs=(vmem, vmem),
        scratch_shapes=[
            pltpu.VMEM((count + 2, slices, tile), bf16),
            pltpu.VMEM((owners, count + 1, per, tile), bf16),
            pltpu.VMEM((owners, count + 1, per, tile), bf16),
            pltpu.VMEM((count, slices, tile), f32),
            pltpu.VMEM((slices, entries, owners, tile), f32),
            pltpu.VMEM((slices * owners, tile), f32),
            pltpu.VMEM((owners, slices, tile), bf16),
            pltpu.VMEM((owners, slices, tile), bf16),
            pltpu.VMEM((owners, count, per, tile), bf16),
            pltpu.VMEM((count, slices, tile), f32),
            pltpu.VMEM((count, slices, tile), bf16),
            pltpu.VMEM((owners, slices, tile), bf16),
            pltpu.VMEM((owners, slices, tile), bf16),
            pltpu.VMEM((slices * owners, tile), f32),
            pltpu.VMEM((slices * places, tile), f32),
            pltpu.VMEM((parts, quarters, own_places, slices // parts, tile), bf16),
            pltpu.VMEM((parts, quarters, own_places, slices // parts, tile), bf16),
            sems((2,)),
            sems((2,)),
            sems((owners,)),
            sems((owners,)),
            sems((owners,)),
            sems((owners,)),
            sems((owners,)),
            sems((owners,)),
            sems((owners,)),
            sems((owners,)),
            sems((parts * quarters,)),
            sems((parts * quarters,)),
            pltpu.VMEM((1, 2 * tile), f32),
            pltpu.VMEM((slices, columns), bf16),
            pltpu.VMEM(image.shape, bf16),
            pltpu.VMEM((slices * places, tile), f32),
            pltpu.VMEM((entries, tile, tile), bf16),
            sems((3,)),
        ],
        compiler_params=pltpu.CompilerParams(
            collective_id=0, has_side_effects=True, vmem_limit_bytes=48 * 1024 * 1024
        ),
    )(
        phase_kernel[None],
        projections,
        image,
        tile_library,
        tile_entry[0],
        tile_image[0],
        tile_slot[0],
        tile_count,
        slot_block[0],
    )
    return residual[None], image_next


def fits_kernel(projections, phase_kernel, image, tile_library, tile_entry, *rest):
    owners, quarters = lax.axis_size("dom"), lax.axis_size("ray")
    tile = tile_library.shape[-1]
    angles, slices, columns = projections.shape
    return (
        angles == 1
        and slices % 16 == 0
        and slices == 8 * owners
        and owners == 8
        and tile == 128
        and phase_kernel.shape[0] == tile + 1
        and columns % tile == 0
        and tile_library.shape[2] % 2 == 0
        and (image.shape[0] // tile) % (16 * 1) == 0
        and (image.shape[0] // tile) % quarters == 0
        and tile_entry.shape[2] <= 256
    )


def any_shards(*args):
    if fits_kernel(*args):
        return fast_shards(*args)
    return shards(*args)


def solution(mesh):
    return jax.shard_map(
        any_shards,
        mesh=mesh,
        in_specs=(
            P("dom", None, "ray"),
            P(),
            P("dom", None),
            P("dom", "ray", None, None, None),
            P("dom", "ray", None),
            P("dom", "ray", None),
            P("dom", "ray", None),
            P("dom", "ray"),
            P("dom", "ray", None),
        ),
        out_specs=(P("dom", None, "ray"), P(("dom", "ray"), None)),
        check_vma=False,
    )
```
